32 devices in a mesh: tm: 8 (over z, y), chan: 4 (over x, core).
Axes of the slice: x: 2, y: 2, z: 4, core: 2. Of those that a mesh axis runs over, the one named last changes fastest.
Arguments:
- series: float32 [256, 2048], P('chan', 'tm'), may hold values from -6 to 6
- lengths: int32 [16], replicated, may hold values from 42 to 128
Outputs:
- peak: float32 [2048], P('tm')
The draws below stay inside these ranges and needn't reach their ends.
All inputs are finite; a program needn't handle non-finite values.
Results may differ from the reference program's by a relative error of at most 0.0015.
Values may be sent and summed in bfloat16 or wider, within the bound.
A program may use at most 128 MiB of HBM per device.

```python
import jax
import jax.numpy as jnp
from jax import lax

C = 256
WIN = 256
ROWS_DEV = 256
STEPS = 2
ROWS = 2048
NSEG = 16
N_TM = 8


def with_ends(drawn, own_key, low, largest):
    longest = drawn.shape.index(max(drawn.shape))
    spots = []
    for shift in (0, 1):
        where = [jax.random.randint(jax.random.fold_in(own_key, axis), (), 0, length) for axis, length in enumerate(drawn.shape)]
        where[longest] = (where[longest] + shift) % drawn.shape[longest]
        spots.append(tuple(where))
    return drawn.at[spots[0]].set(low).at[spots[1]].set(largest)


def block_scale(key, shape, shards, smallest, top_value):
    factor_of = 1.0
    for axis_at, shards_of in shards:
        draws = jax.random.uniform(jax.random.fold_in(jax.random.fold_in(key, 6), axis_at), (shards_of,), jnp.float32, smallest / len(shards), top_value / len(shards))
        factor_of = factor_of * jnp.repeat(jnp.exp(draws), shape[axis_at] // shards_of).reshape((-1,) + (1,) * (len(shape) - 1 - axis_at))
    return factor_of


def normal_values(key, extent, width, bound, pieces=(), held_as=jnp.bfloat16):
    array = jax.random.normal(key, extent, jnp.float32) * width
    if len(pieces) > 0:
        array = block_scale(key, extent, pieces, -0.22, 0.18) * array
    return jnp.clip(array, min=-bound, max=bound).astype(held_as)


def setup_inputs(seed: int = 0) -> dict:
    key_list = jax.random.split(jax.random.key(seed), 3)
    series = normal_values(key_list[0], (C, ROWS), 1.0, 6.0, ((0, 4), (1, 8)), jnp.float32)
    lengths = with_ends(jax.random.randint(key_list[1], (NSEG,), ROWS_DEV // 6, ROWS_DEV // 2 + 1), jax.random.fold_in(key_list[1], 1), ROWS_DEV // 6, (ROWS_DEV // 2 + 1) - 1).astype(jnp.int32)
    return {"series": series, "lengths": lengths}


EPS = 1e-05
MASKED = -1000000000.0

def windows_of(extended):
    count = extended.shape[1] - WIN + 1
    starts = jnp.arange(count, dtype=jnp.int32)
    index = starts[:, None] + jnp.arange(WIN, dtype=jnp.int32)[None, :]
    stacked = jnp.transpose(extended[:, index], (1, 0, 2))
    center = stacked - lax.optimization_barrier(jnp.mean(stacked, axis=2, keepdims=True))
    spread = lax.optimization_barrier(jnp.mean(center * center, axis=2, keepdims=True))
    normed = center * lax.rsqrt(spread + EPS)
    return normed.reshape(count, -1).astype(jnp.bfloat16)

def validity(block, lengths, rows, total):
    local = jnp.arange(rows, dtype=jnp.int32)
    seg_len = rows // 2
    pair = lax.dynamic_slice_in_dim(lengths, (block * 2).astype(jnp.int32), 2)
    limit = jnp.where(local < seg_len, pair[0], pair[1])
    offset = local % seg_len
    return (offset < limit) & (block * rows + local <= total - WIN)

def reference(series, lengths):
    total = series.shape[1]
    padded = jnp.concatenate([series, jnp.zeros((series.shape[0], WIN - 1), series.dtype)], axis=1)
    excl = WIN // 4

    def block_windows(block):
        start = (block * ROWS_DEV).astype(jnp.int32)
        return windows_of(lax.dynamic_slice_in_dim(padded, start, ROWS_DEV + WIN - 1, 1))

    def row_block(block):
        rows_z = block_windows(block)
        rows_ok = validity(block, lengths, ROWS_DEV, total)
        local = jnp.arange(ROWS_DEV, dtype=jnp.int32)
        best = jnp.full((ROWS_DEV,), MASKED, jnp.float32)
        for step in range(STEPS + 1):
            other = block - step
            safe = jnp.maximum(other, 0)
            cols_z = block_windows(safe)
            cols_ok = validity(safe, lengths, ROWS_DEV, total) & (other >= 0)
            score = lax.dot_general(rows_z, cols_z, (((1,), (1,)), ((), ())), preferred_element_type=jnp.float32) * (1.0 / WIN)
            lag = step * ROWS_DEV + local[:, None] - local[None, :]
            keep = rows_ok[:, None] & cols_ok[None, :] & (lag >= excl)
            best = jnp.maximum(best, lax.optimization_barrier(jnp.max(jnp.where(keep, score, MASKED), axis=1)))
        return jnp.where(best > 0.5 * MASKED, best, 0.0).astype(jnp.float32)
    blocks = lax.map(row_block, jnp.arange(N_TM, dtype=jnp.int32))
    return blocks.reshape(total)
```

```python
import functools

import jax
import jax.numpy as jnp
from jax import lax
from jax.experimental import pallas as pl
from jax.experimental.pallas import tpu as pltpu
from jax.sharding import PartitionSpec as P

WIN = 256
STEPS = 2
GROUP = 16
TILE = 32
EPS = 1e-05
MASKED = -1000000000.0
MESH = pl.DeviceIdType.MESH


def kernel(n_tm, n_chan, lengths, series, out, own_x, halo, xt, moments, mu, sc, z0e, z0o, ze, zo, acc,
           send16, recv32, recv16, peaks, load_sem, halo_send, halo_recv, part_send, part_recv, peak_send, peak_recv):
    depth, rows = own_x.shape
    total = rows * n_tm
    excl = WIN // 4
    half = WIN // 2
    lanes = 2 * depth
    chunks = half // GROUP
    heights = [rows - excl] + [rows] * STEPS
    block = lax.axis_index("tm")
    part = lax.axis_index("chan")

    def peer(d):
        return jnp.bitwise_xor(part, d)

    load = pltpu.make_async_copy(series, own_x, load_sem)
    load.start()

    barrier = pltpu.get_barrier_semaphore()
    for distance in (1, -1, -2):
        target = block + distance

        @pl.when((target >= 0) & (target < n_tm))
        def _(target=target):
            pl.semaphore_signal(barrier, inc=1, device_id=(target, part), device_id_type=MESH)

    for d in range(1, n_chan):
        pl.semaphore_signal(barrier, inc=1, device_id=(block, peer(d)), device_id_type=MESH)
    greeted = n_chan - 1
    for distance in (-1, 1, 2):
        target = block + distance
        greeted = greeted + jnp.where((target >= 0) & (target < n_tm), 1, 0)
    pl.semaphore_wait(barrier, greeted)

    reach = (-1, 1, 2)

    def halo_copy(slot):
        return pltpu.make_async_remote_copy(
            src_ref=series, dst_ref=halo.at[slot], send_sem=halo_send.at[slot], recv_sem=halo_recv.at[slot],
            device_id=(block + reach[slot], part), device_id_type=MESH)

    def sends(slot):
        target = block + reach[slot]
        return (target >= 0) & (target < n_tm)

    def receives(slot):
        origin = block - reach[slot]
        return (origin >= 0) & (origin < n_tm)

    def start_halo(slot):
        @pl.when(sends(slot))
        def _():
            halo_copy(slot).start()

    def sent_halo(slot):
        @pl.when(sends(slot))
        def _():
            halo_copy(slot).wait_send()

    def take_halo(slot):
        @pl.when(receives(slot))
        def _():
            halo_copy(slot).wait_recv()

    def place(value, at):
        xt[at:at + half, :] = jnp.concatenate([value[:, :half], value[:, half:]], axis=0).T

    def bridge(at):
        early, late = pltpu.roll(xt[at - half:at, :], depth, 1), pltpu.roll(xt[at + half:at + 2 * half, :], depth, 1)
        lane = lax.broadcasted_iota(jnp.int32, (half, lanes), 1)
        xt[at:at + half, :] = jnp.where(lane < depth, early, late)

    def base(step):
        return (STEPS - step) * rows

    def stats(step):
        lo = base(step)
        hi = lo + rows + (half if step == 0 else 0)
        span, level = 1, 0
        while span < half:
            last = min(hi, (STEPS + 2) * rows - half - 2 * span)
            last = lo + -(-(last - lo) // 8) * 8
            for at in range(lo, last, TILE):
                end = min(at + TILE, last)
                if span == 1:
                    here, later = xt[at:end, :], xt[at + span:end + span, :]
                else:
                    here, later = moments[level - 1, 0, at:end, :], moments[level - 1, 0, at + span:end + span, :]
                gap = later - here
                second = gap * gap * (0.5 / span)
                if span > 1:
                    second = second + (moments[level - 1, 1, at:end, :] + moments[level - 1, 1, at + span:end + span, :])
                moments[level, 0, at:end, :] = here + later
                moments[level, 1, at:end, :] = second
            span, level = 2 * span, level + 1
        for at in range(0, rows, TILE):
            here = moments[level - 1, 0, lo + at:lo + at + TILE, :]
            second = moments[level - 1, 1, lo + at:lo + at + TILE, :]
            later = pltpu.roll(here, depth, 1)
            gap = later - here
            second = second + pltpu.roll(second, depth, 1) + gap * gap * (0.5 / half)
            mu[step, at:at + TILE, :] = (here + later) * (1.0 / WIN)
            sc[step, at:at + TILE, :] = lax.rsqrt(second * (1.0 / WIN) + EPS)

    def build(step, g, target):
        for tile in range(0, rows, 16):
            m, s = mu[step, tile:tile + 16, :], sc[step, tile:tile + 16, :]
            for k in range(GROUP):
                z = (xt[pl.ds(base(step) + g * GROUP + (tile + k), 16), :] - m) * s
                target[k, tile:tile + 16, :] = z.astype(jnp.bfloat16)

    def product(step, weights, target):
        left = jnp.concatenate([target[k, 0:heights[step], :] for k in range(GROUP)], axis=1)
        right = jnp.concatenate([weights[k] for k in range(GROUP)], axis=1)
        return lax.dot_general(left, right, (((1,), (1,)), ((), ())), preferred_element_type=jnp.float32)

    def send(step):
        own = heights[step] // n_chan
        copies = []
        for d in range(1, n_chan):
            at = pl.ds(pl.multiple_of(peer(d) * own, own), own)
            if d == 1:
                src, dst = acc.at[step, at, :], recv32.at[step, 0:own, :]
            else:
                send16[step, d - 2, 0:own, :] = acc[step, at, :].astype(jnp.bfloat16)
                src, dst = send16.at[step, d - 2, 0:own, :], recv16.at[step, d - 2, 0:own, :]
            copy = pltpu.make_async_remote_copy(
                src_ref=src, dst_ref=dst, send_sem=part_send.at[step, d - 1], recv_sem=part_recv.at[step, d - 1],
                device_id=(block, peer(d)), device_id_type=MESH)
            copy.start()
            copies.append(copy)
        return copies

    start_halo(0)
    load.wait()
    place(own_x[...], STEPS * rows)
    pad = xt.shape[0] - ((STEPS + 2) * rows - half)
    xt[xt.shape[0] - pad:, :] = jnp.zeros((pad, lanes), jnp.float32)
    acc[...] = jnp.zeros_like(acc)
    sent_halo(0)
    start_halo(1)
    take_halo(0)
    start_halo(2)

    def arrive(step):
        if step == 0:
            place(jnp.where(block == n_tm - 1, 0.0, halo[0]), (STEPS + 1) * rows)
        else:
            take_halo(step)
            place(halo[step], base(step))
        bridge(base(step) + half)

    sent = []
    pairs = chunks // 2
    for step in range(STEPS + 1):
        arrive(step)
        stats(step)
        if step == 0:
            build(0, 0, z0e.at[0])
        else:
            build(step, 0, ze)

        def chunk(h, carry, step=step):
            first, second = (z0e.at[h], z0o.at[h]) if step == 0 else (ze, zo)
            a = product(step, z0e.at[h], first)
            build(step, 2 * h + 1, second)
            following = jnp.minimum(h + 1, pairs - 1)
            if step == 0:
                b = product(step, z0o.at[h], second)
                build(step, 2 * h + 2, z0e.at[h + 1])
            else:
                b = product(step, z0o.at[h], second)
                build(step, 2 * h + 2, ze)
            acc[step, 0:heights[step], :] += a + b
            return carry

        lax.fori_loop(0, pairs, chunk, 0)
        sent.append(send(step))

    lane_at = lax.broadcasted_iota(jnp.int32, (1, rows), 1)

    def valid(which, local):
        seg_len = rows // 2
        limit = jnp.where(local < seg_len, lengths[which * 2], lengths[which * 2 + 1])
        offset = jnp.where(local < seg_len, local, local - seg_len)
        return (offset < limit) & (which * rows + local <= total - WIN)

    best = None
    for step in range(STEPS + 1):
        own = heights[step] // n_chan
        row_at = part * own + lax.broadcasted_iota(jnp.int32, (own, rows), 0)
        other = block - step
        safe = jnp.maximum(other, 0)
        col_at = lax.broadcasted_iota(jnp.int32, (own, rows), 1)
        keep = valid(block, col_at) & valid(safe, row_at) & (other >= 0) & (step * rows + col_at - row_at >= excl)
        for copy in sent[step]:
            copy.wait_recv()
        summed = acc[step, pl.ds(pl.multiple_of(part * own, own), own), :] + recv32[step, 0:own, :]
        for d in range(2, n_chan):
            summed = summed + recv16[step, d - 2, 0:own, :].astype(jnp.float32)
        top = jnp.max(jnp.where(keep, summed * (1.0 / WIN), MASKED), axis=0, keepdims=True)
        best = top if best is None else jnp.maximum(best, top)
    peaks[0] = best
    copies = []
    for d in range(1, n_chan):
        copy = pltpu.make_async_remote_copy(
            src_ref=peaks.at[0], dst_ref=peaks.at[d], send_sem=peak_send.at[d - 1], recv_sem=peak_recv.at[d - 1],
            device_id=(block, peer(d)), device_id_type=MESH)
        copy.start()
        copies.append(copy)
    for copy in copies:
        copy.wait_recv()
    for d in range(1, n_chan):
        best = jnp.maximum(best, peaks[d])
    out[...] = jnp.where(best > 0.5 * MASKED, best, 0.0)

    sent_halo(1)
    sent_halo(2)
    for copy in [c for step in sent for c in step] + copies:
        copy.wait_send()


def solution(mesh):
    n_tm, n_chan = mesh.shape["tm"], mesh.shape["chan"]

    def body(series, lengths):
        depth, rows = series.shape
        half = WIN // 2
        lanes = 2 * depth
        pairs = half // GROUP // 2
        high = (STEPS + 2) * rows - half + 16 + GROUP
        levels = half.bit_length() - 1
        own = rows // n_chan
        vmem = pl.BlockSpec(memory_space=pltpu.VMEM)
        peak = pl.pallas_call(
            functools.partial(kernel, n_tm, n_chan),
            out_shape=jax.ShapeDtypeStruct((1, rows), jnp.float32),
            in_specs=[pl.BlockSpec(memory_space=pltpu.SMEM), pl.BlockSpec(memory_space=pl.ANY)],
            out_specs=vmem,
            scratch_shapes=[
                pltpu.VMEM((depth, rows), jnp.float32),
                pltpu.VMEM((STEPS + 1, depth, rows), jnp.float32),
                pltpu.VMEM((high, lanes), jnp.float32),
                pltpu.VMEM((levels, 2, high, lanes), jnp.float32),
                pltpu.VMEM((STEPS + 1, rows, lanes), jnp.float32),
                pltpu.VMEM((STEPS + 1, rows, lanes), jnp.float32),
                pltpu.VMEM((pairs + 1, GROUP, rows, lanes), jnp.bfloat16),
                pltpu.VMEM((pairs, GROUP, rows, lanes), jnp.bfloat16),
                pltpu.VMEM((GROUP, rows, lanes), jnp.bfloat16),
                pltpu.VMEM((GROUP, rows, lanes), jnp.bfloat16),
                pltpu.VMEM((STEPS + 1, rows, rows), jnp.float32),
                pltpu.VMEM((STEPS + 1, n_chan - 2, own, rows), jnp.bfloat16),
                pltpu.VMEM((STEPS + 1, own, rows), jnp.float32),
                pltpu.VMEM((STEPS + 1, n_chan - 2, own, rows), jnp.bfloat16),
                pltpu.VMEM((n_chan, 1, rows), jnp.float32),
                pltpu.SemaphoreType.DMA,
                pltpu.SemaphoreType.DMA((STEPS + 1,)),
                pltpu.SemaphoreType.DMA((STEPS + 1,)),
                pltpu.SemaphoreType.DMA((STEPS + 1, n_chan - 1)),
                pltpu.SemaphoreType.DMA((STEPS + 1, n_chan - 1)),
                pltpu.SemaphoreType.DMA((n_chan - 1,)),
                pltpu.SemaphoreType.DMA((n_chan - 1,)),
            ],
            compiler_params=pltpu.CompilerParams(collective_id=0, has_side_effects=True),
        )(lengths, series)
        return peak.reshape(rows)

    return jax.shard_map(
        body, mesh=mesh, in_specs=(P("chan", "tm"), P()), out_specs=P("tm"), check_vma=False)
```

```python
import functools

import jax
import jax.numpy as jnp
from jax import lax
from jax.experimental import pallas as pl
from jax.experimental.pallas import tpu as pltpu
from jax.sharding import PartitionSpec as P

WIN = 256
STEPS = 2
GROUP = 16
TILE = 32
EPS = 1e-05
MASKED = -1000000000.0
MESH = pl.DeviceIdType.MESH


def kernel(n_tm, n_chan, lengths_in, series, out, lengths, own_x, halo, xt, moments, mu, sc, z0e, z0o, z1e, z1o, z2e, z2o,
           acc, send16, recv32, recv16, peaks, load_sem, lengths_sem, halo_send, halo_recv, part_send, part_recv, peak_send, peak_recv):
    depth, rows = own_x.shape
    total = rows * n_tm
    excl = WIN // 4
    half = WIN // 2
    lanes = 2 * depth
    chunks = half // GROUP
    heights = [rows - excl] + [rows] * STEPS
    block = lax.axis_index("tm")
    part = lax.axis_index("chan")

    def peer(d):
        return jnp.bitwise_xor(part, d)

    load = pltpu.make_async_copy(series, own_x, load_sem)
    load.start()
    load_lengths = pltpu.make_async_copy(lengths_in, lengths, lengths_sem)
    load_lengths.start()

    barrier = pltpu.get_barrier_semaphore()
    for distance in (1, -1, -2):
        target = block + distance

        @pl.when((target >= 0) & (target < n_tm))
        def _(target=target):
            pl.semaphore_signal(barrier, inc=1, device_id=(target, part), device_id_type=MESH)

    for d in range(1, n_chan):
        pl.semaphore_signal(barrier, inc=1, device_id=(block, peer(d)), device_id_type=MESH)
    greeted = n_chan - 1
    for distance in (-1, 1, 2):
        target = block + distance
        greeted = greeted + jnp.where((target >= 0) & (target < n_tm), 1, 0)
    pl.semaphore_wait(barrier, greeted)

    reach = (-1, 1, 2)

    def halo_copy(slot):
        return pltpu.make_async_remote_copy(
            src_ref=series, dst_ref=halo.at[slot], send_sem=halo_send.at[slot], recv_sem=halo_recv.at[slot],
            device_id=(block + reach[slot], part), device_id_type=MESH)

    def sends(slot):
        target = block + reach[slot]
        return (target >= 0) & (target < n_tm)

    def receives(slot):
        origin = block - reach[slot]
        return (origin >= 0) & (origin < n_tm)

    def start_halo(slot):
        @pl.when(sends(slot))
        def _():
            halo_copy(slot).start()

    def sent_halo(slot):
        @pl.when(sends(slot))
        def _():
            halo_copy(slot).wait_send()

    def take_halo(slot):
        @pl.when(receives(slot))
        def _():
            halo_copy(slot).wait_recv()

    def place(value, at):
        xt[at:at + half, :] = jnp.concatenate([value[:, :half], value[:, half:]], axis=0).T

    def bridge(at):
        early, late = pltpu.roll(xt[at - half:at, :], depth, 1), pltpu.roll(xt[at + half:at + 2 * half, :], depth, 1)
        lane = lax.broadcasted_iota(jnp.int32, (half, lanes), 1)
        xt[at:at + half, :] = jnp.where(lane < depth, early, late)

    def base(step):
        return (STEPS - step) * rows

    def stats(step):
        lo = base(step)
        hi = lo + rows + (half if step == 0 else 0)
        span, level = 1, 0
        while span < half:
            last = min(hi, (STEPS + 2) * rows - half - 2 * span)
            last = lo + -(-(last - lo) // 8) * 8
            for at in range(lo, last, TILE):
                end = min(at + TILE, last)
                if span == 1:
                    here, later = xt[at:end, :], xt[at + span:end + span, :]
                else:
                    here, later = moments[level - 1, 0, at:end, :], moments[level - 1, 0, at + span:end + span, :]
                gap = later - here
                second = gap * gap * (0.5 / span)
                if span > 1:
                    second = second + (moments[level - 1, 1, at:end, :] + moments[level - 1, 1, at + span:end + span, :])
                moments[level, 0, at:end, :] = here + later
                moments[level, 1, at:end, :] = second
            span, level = 2 * span, level + 1
        for at in range(0, rows, TILE):
            here = moments[level - 1, 0, lo + at:lo + at + TILE, :]
            second = moments[level - 1, 1, lo + at:lo + at + TILE, :]
            later = pltpu.roll(here, depth, 1)
            gap = later - here
            second = second + pltpu.roll(second, depth, 1) + gap * gap * (0.5 / half)
            mu[step, at:at + TILE, :] = (here + later) * (1.0 / WIN)
            sc[step, at:at + TILE, :] = lax.rsqrt(second * (1.0 / WIN) + EPS)

    def build(step, g, target):
        for tile in range(0, rows, 16):
            m, s = mu[step, tile:tile + 16, :], sc[step, tile:tile + 16, :]
            for k in range(GROUP):
                z = (xt[pl.ds(base(step) + g * GROUP + (tile + k), 16), :] - m) * s
                target[k, tile:tile + 16, :] = z.astype(jnp.bfloat16)

    def product(weights, streamed):
        left = jnp.concatenate(
            [jnp.concatenate([z[k, 0:height, :] for z, height in streamed], axis=0) for k in range(GROUP)], axis=1)
        right = jnp.concatenate([weights[k] for k in range(GROUP)], axis=1)
        return lax.dot_general(left, right, (((1,), (1,)), ((), ())), preferred_element_type=jnp.float32)

    def send(step):
        own = heights[step] // n_chan
        copies = []
        for d in range(1, n_chan):
            at = pl.ds(pl.multiple_of(peer(d) * own, own), own)
            if d == 1:
                src, dst = acc.at[step, at, :], recv32.at[step, 0:own, :]
            else:
                send16[step, d - 2, 0:own, :] = acc[step, at, :].astype(jnp.bfloat16)
                src, dst = send16.at[step, d - 2, 0:own, :], recv16.at[step, d - 2, 0:own, :]
            copy = pltpu.make_async_remote_copy(
                src_ref=src, dst_ref=dst, send_sem=part_send.at[step, d - 1], recv_sem=part_recv.at[step, d - 1],
                device_id=(block, peer(d)), device_id_type=MESH)
            copy.start()
            copies.append(copy)
        return copies

    start_halo(0)
    load.wait()
    place(own_x[...], STEPS * rows)
    pad = xt.shape[0] - ((STEPS + 2) * rows - half)
    xt[xt.shape[0] - pad:, :] = jnp.zeros((pad, lanes), jnp.float32)
    acc[...] = jnp.zeros_like(acc)
    sent_halo(0)
    start_halo(1)
    take_halo(0)
    start_halo(2)

    def arrive(step):
        if step == 0:
            place(jnp.where(block == n_tm - 1, 0.0, halo[0]), (STEPS + 1) * rows)
        else:
            if step == 1:
                take_halo(step)
            place(halo[step], base(step))
        bridge(base(step) + half)

    sent = []
    pairs = chunks // 2
    low, mid = heights[0], heights[0] + heights[1]

    def add_near(value):
        acc[0, 0:low, :] += value[:low]
        acc[1, 0:heights[1], :] += value[low:mid]

    for step in range(2):
        arrive(step)
        stats(step)
        build(step, 0, z0e.at[0] if step == 0 else z1e)

    def near(h, carry):
        first = product(z0e.at[h], [(z0e.at[h], low), (z1e, heights[1])])
        build(0, 2 * h + 1, z0o.at[h])
        build(1, 2 * h + 1, z1o)
        second = product(z0o.at[h], [(z0o.at[h], low), (z1o, heights[1])])
        build(0, 2 * h + 2, z0e.at[h + 1])
        build(1, 2 * h + 2, z1e)
        add_near(first + second)
        return carry

    lax.fori_loop(0, pairs - 1, near, 0)
    take_halo(2)
    last = pairs - 1
    first = product(z0e.at[last], [(z0e.at[last], low), (z1e, heights[1])])
    build(0, 2 * last + 1, z0o.at[last])
    build(1, 2 * last + 1, z1o)
    second = product(z0o.at[last], [(z0o.at[last], low), (z1o, heights[1])])
    arrive(2)
    stats(2)
    build(2, 0, z2e)
    add_near(first + second)
    sent.append(send(0))
    sent.append(send(1))

    def far(h, carry):
        first = product(z0e.at[h], [(z2e, heights[2])])
        build(2, 2 * h + 1, z2o)
        second = product(z0o.at[h], [(z2o, heights[2])])
        build(2, 2 * h + 2, z2e)
        acc[2] += first + second
        return carry

    lax.fori_loop(0, pairs, far, 0)
    sent.append(send(2))

    load_lengths.wait()

    def valid(which, local):
        seg_len = rows // 2
        limit = jnp.where(local < seg_len, lengths[which * 2], lengths[which * 2 + 1])
        offset = jnp.where(local < seg_len, local, local - seg_len)
        return (offset < limit) & (which * rows + local <= total - WIN)

    best = None
    for step in range(STEPS + 1):
        own = heights[step] // n_chan
        row_at = part * own + lax.broadcasted_iota(jnp.int32, (own, rows), 0)
        other = block - step
        safe = jnp.maximum(other, 0)
        col_at = lax.broadcasted_iota(jnp.int32, (own, rows), 1)
        keep = valid(block, col_at) & valid(safe, row_at) & (other >= 0) & (step * rows + col_at - row_at >= excl)
        for copy in sent[step]:
            copy.wait_recv()
        summed = acc[step, pl.ds(pl.multiple_of(part * own, own), own), :] + recv32[step, 0:own, :]
        for d in range(2, n_chan):
            summed = summed + recv16[step, d - 2, 0:own, :].astype(jnp.float32)
        top = jnp.max(jnp.where(keep, summed * (1.0 / WIN), MASKED), axis=0, keepdims=True)
        best = top if best is None else jnp.maximum(best, top)
    peaks[0] = best
    copies = []
    for d in range(1, n_chan):
        copy = pltpu.make_async_remote_copy(
            src_ref=peaks.at[0], dst_ref=peaks.at[d], send_sem=peak_send.at[d - 1], recv_sem=peak_recv.at[d - 1],
            device_id=(block, peer(d)), device_id_type=MESH)
        copy.start()
        copies.append(copy)
    for copy in copies:
        copy.wait_recv()
    for d in range(1, n_chan):
        best = jnp.maximum(best, peaks[d])
    out[...] = jnp.where(best > 0.5 * MASKED, best, 0.0)

    sent_halo(1)
    sent_halo(2)
    for copy in [c for step in sent for c in step] + copies:
        copy.wait_send()


def solution(mesh):
    n_tm, n_chan = mesh.shape["tm"], mesh.shape["chan"]

    def body(series, lengths):
        depth, rows = series.shape
        half = WIN // 2
        lanes = 2 * depth
        pairs = half // GROUP // 2
        high = (STEPS + 2) * rows - half + 16 + GROUP
        levels = half.bit_length() - 1
        own = rows // n_chan
        vmem = pl.BlockSpec(memory_space=pltpu.VMEM)
        peak = pl.pallas_call(
            functools.partial(kernel, n_tm, n_chan),
            out_shape=pltpu.VMEM((1, rows), jnp.float32),
            in_specs=[pl.BlockSpec(memory_space=pl.ANY), pl.BlockSpec(memory_space=pl.ANY)],
            out_specs=vmem,
            scratch_shapes=[
                pltpu.SMEM(lengths.shape, jnp.int32),
                pltpu.VMEM((depth, rows), jnp.float32),
                pltpu.VMEM((STEPS + 1, depth, rows), jnp.float32),
                pltpu.VMEM((high, lanes), jnp.float32),
                pltpu.VMEM((levels, 2, high, lanes), jnp.float32),
                pltpu.VMEM((STEPS + 1, rows, lanes), jnp.float32),
                pltpu.VMEM((STEPS + 1, rows, lanes), jnp.float32),
                pltpu.VMEM((pairs + 1, GROUP, rows, lanes), jnp.bfloat16),
                pltpu.VMEM((pairs, GROUP, rows, lanes), jnp.bfloat16),
                pltpu.VMEM((GROUP, rows, lanes), jnp.bfloat16),
                pltpu.VMEM((GROUP, rows, lanes), jnp.bfloat16),
                pltpu.VMEM((GROUP, rows, lanes), jnp.bfloat16),
                pltpu.VMEM((GROUP, rows, lanes), jnp.bfloat16),
                pltpu.VMEM((STEPS + 1, rows, rows), jnp.float32),
                pltpu.VMEM((STEPS + 1, n_chan - 2, own, rows), jnp.bfloat16),
                pltpu.VMEM((STEPS + 1, own, rows), jnp.float32),
                pltpu.VMEM((STEPS + 1, n_chan - 2, own, rows), jnp.bfloat16),
                pltpu.VMEM((n_chan, 1, rows), jnp.float32),
                pltpu.SemaphoreType.DMA,
                pltpu.SemaphoreType.DMA,
                pltpu.SemaphoreType.DMA((STEPS + 1,)),
                pltpu.SemaphoreType.DMA((STEPS + 1,)),
                pltpu.SemaphoreType.DMA((STEPS + 1, n_chan - 1)),
                pltpu.SemaphoreType.DMA((STEPS + 1, n_chan - 1)),
                pltpu.SemaphoreType.DMA((n_chan - 1,)),
                pltpu.SemaphoreType.DMA((n_chan - 1,)),
            ],
            compiler_params=pltpu.CompilerParams(collective_id=0, has_side_effects=True),
        )(lengths, series)
        return peak.reshape(rows)

    return jax.shard_map(
        body, mesh=mesh, in_specs=(P("chan", "tm"), P()), out_specs=P("tm"), check_vma=False)
```

```python
import functools

import jax
import jax.numpy as jnp
from jax import lax
from jax.experimental import pallas as pl
from jax.experimental.pallas import tpu as pltpu
from jax.sharding import PartitionSpec as P

WIN = 256
STEPS = 2
GROUP = 16
TILE = 32
EARLY = 2
EPS = 1e-05
MASKED = -1000000000.0
MESH = pl.DeviceIdType.MESH


def kernel(n_tm, n_chan, lengths_in, series, out, lengths, own_x, halo, xt, moments, mu, sc, z0e, z0o, z1e, z1o, z2e, z2o,
           acc, send16, recv32, recv16, peaks, load_sem, lengths_sem, halo_send, halo_recv, part_send, part_recv, peak_send, peak_recv):
    depth, rows = own_x.shape
    total = rows * n_tm
    excl = WIN // 4
    half = WIN // 2
    lanes = 2 * depth
    chunks = half // GROUP
    heights = [rows - excl] + [rows] * STEPS
    block = lax.axis_index("tm")
    part = lax.axis_index("chan")

    def peer(d):
        return jnp.bitwise_xor(part, d)

    load = pltpu.make_async_copy(series, own_x, load_sem)
    load.start()
    load_lengths = pltpu.make_async_copy(lengths_in, lengths, lengths_sem)
    load_lengths.start()

    barrier = pltpu.get_barrier_semaphore()
    for distance in (1, -1, -2):
        target = block + distance

        @pl.when((target >= 0) & (target < n_tm))
        def _(target=target):
            pl.semaphore_signal(barrier, inc=1, device_id=(target, part), device_id_type=MESH)

    for d in range(1, n_chan):
        pl.semaphore_signal(barrier, inc=1, device_id=(block, peer(d)), device_id_type=MESH)
    greeted = n_chan - 1
    for distance in (-1, 1, 2):
        target = block + distance
        greeted = greeted + jnp.where((target >= 0) & (target < n_tm), 1, 0)
    pl.semaphore_wait(barrier, greeted)

    reach = (-1, 1, 2)

    def halo_copy(slot):
        return pltpu.make_async_remote_copy(
            src_ref=own_x, dst_ref=halo.at[slot], send_sem=halo_send.at[slot], recv_sem=halo_recv.at[slot],
            device_id=(block + reach[slot], part), device_id_type=MESH)

    def sends(slot):
        target = block + reach[slot]
        return (target >= 0) & (target < n_tm)

    def receives(slot):
        origin = block - reach[slot]
        return (origin >= 0) & (origin < n_tm)

    def start_halo(slot):
        @pl.when(sends(slot))
        def _():
            halo_copy(slot).start()

    def sent_halo(slot):
        @pl.when(sends(slot))
        def _():
            halo_copy(slot).wait_send()

    def take_halo(slot):
        @pl.when(receives(slot))
        def _():
            halo_copy(slot).wait_recv()

    def place(upper, lower, at):
        xt[at:at + half, :] = jnp.concatenate([upper, lower], axis=0).T

    def base(step):
        return (STEPS - step) * rows

    def stats(step):
        lo = base(step)
        hi = lo + rows + (half if step == 0 else 0)
        span, level = 1, 0
        while span < half:
            last = min(hi, (STEPS + 2) * rows - half - 2 * span)
            last = lo + -(-(last - lo) // 8) * 8
            for at in range(lo, last, TILE):
                end = min(at + TILE, last)
                if span == 1:
                    here, later = xt[at:end, :], xt[at + span:end + span, :]
                else:
                    here, later = moments[level - 1, 0, at:end, :], moments[level - 1, 0, at + span:end + span, :]
                gap = later - here
                second = gap * gap * (0.5 / span)
                if span > 1:
                    second = second + (moments[level - 1, 1, at:end, :] + moments[level - 1, 1, at + span:end + span, :])
                moments[level, 0, at:end, :] = here + later
                moments[level, 1, at:end, :] = second
            span, level = 2 * span, level + 1
        for at in range(0, rows, TILE):
            here = moments[level - 1, 0, lo + at:lo + at + TILE, :]
            second = moments[level - 1, 1, lo + at:lo + at + TILE, :]
            later = pltpu.roll(here, depth, 1)
            gap = later - here
            second = second + pltpu.roll(second, depth, 1) + gap * gap * (0.5 / half)
            mu[step, at:at + TILE, :] = (here + later) * (1.0 / WIN)
            sc[step, at:at + TILE, :] = lax.rsqrt(second * (1.0 / WIN) + EPS)

    def build(step, g, target):
        for tile in range(0, rows, 16):
            m, s = mu[step, tile:tile + 16, :], sc[step, tile:tile + 16, :]
            for k in range(GROUP):
                z = (xt[pl.ds(base(step) + g * GROUP + (tile + k), 16), :] - m) * s
                target[k, tile:tile + 16, :] = z.astype(jnp.bfloat16)

    def product(weights, streamed):
        left = jnp.concatenate(
            [jnp.concatenate([z[k, 0:height, :] for z, height in streamed], axis=0) for k in range(GROUP)], axis=1)
        right = jnp.concatenate([weights[k] for k in range(GROUP)], axis=1)
        return lax.dot_general(left, right, (((1,), (1,)), ((), ())), preferred_element_type=jnp.float32)

    def send(step):
        own = heights[step] // n_chan
        copies = []
        for d in [*range(2, n_chan), 1]:
            at = pl.ds(pl.multiple_of(peer(d) * own, own), own)
            if d == 1:
                src, dst = acc.at[step, at, :], recv32.at[step, 0:own, :]
            else:
                send16[step, d - 2, 0:own, :] = acc[step, at, :].astype(jnp.bfloat16)
                src, dst = send16.at[step, d - 2, 0:own, :], recv16.at[step, d - 2, 0:own, :]
            copy = pltpu.make_async_remote_copy(
                src_ref=src, dst_ref=dst, send_sem=part_send.at[step, d - 1], recv_sem=part_recv.at[step, d - 1],
                device_id=(block, peer(d)), device_id_type=MESH)
            copy.start()
            copies.append(copy)
        return copies

    load.wait()
    start_halo(0)
    place(own_x[:, :half], own_x[:, half:], base(0))
    pad = xt.shape[0] - ((STEPS + 2) * rows - half)
    xt[xt.shape[0] - pad:, :] = jnp.zeros((pad, lanes), jnp.float32)
    acc[...] = jnp.zeros_like(acc)
    sent_halo(0)
    start_halo(1)
    start_halo(2)
    take_halo(0)

    def arrive(step):
        if step == 0:
            early, late = own_x, jnp.where(block == n_tm - 1, 0.0, halo[0])
            place(late[:, :half], late[:, half:], base(0) + rows)
            place(early[:, half:], late[:, :half], base(0) + half)
        else:
            early, late = halo[step], own_x if step == 1 else halo[1]
            place(early[:, :half], early[:, half:], base(step))
            place(early[:, half:], late[:, :half], base(step) + half)

    sent = []
    pairs = chunks // 2
    low, mid = heights[0], heights[0] + heights[1]

    take = (low, heights[1], heights[2])

    def near(weights, mine, previous):
        return product(weights, [(mine, take[0]), (previous, take[1])])

    for step in range(2):
        if step == 1:
            take_halo(1)
        arrive(step)
        stats(step)
        build(step, 0, z0e.at[0] if step == 0 else z1e)
    take_halo(2)

    def add_near(first, second, fresh=False):
        for step, lo, hi in ((0, 0, low), (1, low, mid)):
            value = first[lo:hi] + second[lo:hi]
            acc[step, 0:hi - lo, :] = value if fresh else acc[step, 0:hi - lo, :] + value

    for h in range(EARLY):
        first = near(z0e.at[h], z0e.at[h], z1e)
        build(0, 2 * h + 1, z0o.at[h])
        build(1, 2 * h + 1, z1o)
        if h == 0:
            arrive(2)
        second = near(z0o.at[h], z0o.at[h], z1o)
        build(0, 2 * h + 2, z0e.at[h + 1])
        build(1, 2 * h + 2, z1e)
        if h == 0:
            stats(2)
        if h == EARLY - 1:
            build(2, 2 * h + 2, z2e)
        add_near(first, second, h == 0)

    def every(h, carry):
        first = product(z0e.at[h], [(z0e.at[h], take[0]), (z1e, take[1]), (z2e, take[2])])
        build(0, 2 * h + 1, z0o.at[h])
        build(1, 2 * h + 1, z1o)
        build(2, 2 * h + 1, z2o)
        second = product(z0o.at[h], [(z0o.at[h], take[0]), (z1o, take[1]), (z2o, take[2])])
        build(0, 2 * h + 2, z0e.at[h + 1])
        build(1, 2 * h + 2, z1e)
        build(2, lax.rem(2 * h + 2, chunks), z2e)
        add_near(first, second)
        acc[2] += first[mid:] + second[mid:]
        return carry

    lax.fori_loop(EARLY, pairs, every, 0)
    sent.append(send(0))
    sent.append(send(1))

    def far(h, carry):
        first = product(z0e.at[h], [(z2e, take[2])])
        build(2, 2 * h + 1, z2o)
        second = product(z0o.at[h], [(z2o, take[2])])
        build(2, 2 * h + 2, z2e)
        acc[2] += first + second
        return carry

    lax.fori_loop(0, EARLY, far, 0)
    sent.append(send(2))

    load_lengths.wait()

    def valid(which, local):
        seg_len = rows // 2
        limit = jnp.where(local < seg_len, lengths[which * 2], lengths[which * 2 + 1])
        offset = jnp.where(local < seg_len, local, local - seg_len)
        return (offset < limit) & (which * rows + local <= total - WIN)

    best = None
    for step in range(STEPS + 1):
        own = heights[step] // n_chan
        row_at = part * own + lax.broadcasted_iota(jnp.int32, (own, rows), 0)
        other = block - step
        safe = jnp.maximum(other, 0)
        col_at = lax.broadcasted_iota(jnp.int32, (own, rows), 1)
        keep = valid(block, col_at) & valid(safe, row_at) & (other >= 0) & (step * rows + col_at - row_at >= excl)
        for copy in sent[step]:
            copy.wait_recv()
        summed = acc[step, pl.ds(pl.multiple_of(part * own, own), own), :] + recv32[step, 0:own, :]
        for d in range(2, n_chan):
            summed = summed + recv16[step, d - 2, 0:own, :].astype(jnp.float32)
        top = jnp.max(jnp.where(keep, summed * (1.0 / WIN), MASKED), axis=0, keepdims=True)
        best = top if best is None else jnp.maximum(best, top)
    peaks[0] = best
    copies = []
    for d in range(1, n_chan):
        copy = pltpu.make_async_remote_copy(
            src_ref=peaks.at[0], dst_ref=peaks.at[d], send_sem=peak_send.at[d - 1], recv_sem=peak_recv.at[d - 1],
            device_id=(block, peer(d)), device_id_type=MESH)
        copy.start()
        copies.append(copy)
    for slot in range(1, STEPS + 1):
        sent_halo(slot)
    for copy in [c for step in sent for c in step]:
        copy.wait_send()
    for copy in copies:
        copy.wait_recv()
    for d in range(1, n_chan):
        best = jnp.maximum(best, peaks[d])
    out[...] = jnp.where(best > 0.5 * MASKED, best, 0.0)

    for copy in copies:
        copy.wait_send()


def solution(mesh):
    n_tm, n_chan = mesh.shape["tm"], mesh.shape["chan"]

    def body(series, lengths):
        depth, rows = series.shape
        half = WIN // 2
        lanes = 2 * depth
        pairs = half // GROUP // 2
        high = (STEPS + 2) * rows - half + 16 + GROUP
        levels = half.bit_length() - 1
        own = rows // n_chan
        vmem = pl.BlockSpec(memory_space=pltpu.VMEM)
        peak = pl.pallas_call(
            functools.partial(kernel, n_tm, n_chan),
            out_shape=pltpu.VMEM((1, rows), jnp.float32),
            in_specs=[pl.BlockSpec(memory_space=pl.ANY), pl.BlockSpec(memory_space=pl.ANY)],
            out_specs=vmem,
            scratch_shapes=[
                pltpu.SMEM(lengths.shape, jnp.int32),
                pltpu.VMEM((depth, rows), jnp.float32),
                pltpu.VMEM((STEPS + 1, depth, rows), jnp.float32),
                pltpu.VMEM((high, lanes), jnp.float32),
                pltpu.VMEM((levels, 2, high, lanes), jnp.float32),
                pltpu.VMEM((STEPS + 1, rows, lanes), jnp.float32),
                pltpu.VMEM((STEPS + 1, rows, lanes), jnp.float32),
                pltpu.VMEM((pairs + 1, GROUP, rows, lanes), jnp.bfloat16),
                pltpu.VMEM((pairs, GROUP, rows, lanes), jnp.bfloat16),
                pltpu.VMEM((GROUP, rows, lanes), jnp.bfloat16),
                pltpu.VMEM((GROUP, rows, lanes), jnp.bfloat16),
                pltpu.VMEM((GROUP, rows, lanes), jnp.bfloat16),
                pltpu.VMEM((GROUP, rows, lanes), jnp.bfloat16),
                pltpu.VMEM((STEPS + 1, rows, rows), jnp.float32),
                pltpu.VMEM((STEPS + 1, n_chan - 2, own, rows), jnp.bfloat16),
                pltpu.VMEM((STEPS + 1, own, rows), jnp.float32),
                pltpu.VMEM((STEPS + 1, n_chan - 2, own, rows), jnp.bfloat16),
                pltpu.VMEM((n_chan, 1, rows), jnp.float32),
                pltpu.SemaphoreType.DMA,
                pltpu.SemaphoreType.DMA,
                pltpu.SemaphoreType.DMA((STEPS + 1,)),
                pltpu.SemaphoreType.DMA((STEPS + 1,)),
                pltpu.SemaphoreType.DMA((STEPS + 1, n_chan - 1)),
                pltpu.SemaphoreType.DMA((STEPS + 1, n_chan - 1)),
                pltpu.SemaphoreType.DMA((n_chan - 1,)),
                pltpu.SemaphoreType.DMA((n_chan - 1,)),
            ],
            compiler_params=pltpu.CompilerParams(collective_id=0, has_side_effects=True),
        )(lengths, series)
        return peak.reshape(rows)

    return jax.shard_map(
        body, mesh=mesh, in_specs=(P("chan", "tm"), P()), out_specs=P("tm"), check_vma=False)
```

```python
import functools

import jax
import jax.numpy as jnp
from jax import lax
from jax.experimental import pallas as pl
from jax.experimental.pallas import tpu as pltpu
from jax.sharding import PartitionSpec as P

WIN = 256
STEPS = 2
GROUP = 16
TILE = 32
EARLY = 2
EPS = 1e-05
MASKED = -1000000000.0
MESH = pl.DeviceIdType.MESH


def kernel(n_tm, n_chan, lengths_in, series, out, lengths, own_x, halo, xt, moments, mu, sc, z0e, z0o, z1e, z1o, z2e, z2o,
           acc, send16, recv32, recv16, peaks, load_sem, lengths_sem, halo_send, halo_recv, part_send, part_recv, peak_send, peak_recv):
    depth, rows = own_x.shape
    total = rows * n_tm
    excl = WIN // 4
    half = WIN // 2
    lanes = 2 * depth
    chunks = half // GROUP
    heights = [rows - excl] + [rows] * STEPS
    block = lax.axis_index("tm")
    part = lax.axis_index("chan")

    def peer(d):
        return jnp.bitwise_xor(part, d)

    load = pltpu.make_async_copy(series, own_x, load_sem)
    load.start()
    load_lengths = pltpu.make_async_copy(lengths_in, lengths, lengths_sem)
    load_lengths.start()

    barrier = pltpu.get_barrier_semaphore()
    for distance in (1, -1, -2):
        target = block + distance

        @pl.when((target >= 0) & (target < n_tm))
        def _(target=target):
            pl.semaphore_signal(barrier, inc=1, device_id=(target, part), device_id_type=MESH)

    for d in range(1, n_chan):
        pl.semaphore_signal(barrier, inc=1, device_id=(block, peer(d)), device_id_type=MESH)
    greeted = n_chan - 1
    for distance in (-1, 1, 2):
        target = block + distance
        greeted = greeted + jnp.where((target >= 0) & (target < n_tm), 1, 0)
    pl.semaphore_wait(barrier, greeted)

    reach = (-1, -1, 1, 2)
    pieces = ((0, 0, depth // 2), (0, depth // 2, depth), (1, 0, depth), (2, 0, depth))

    def halo_copy(i):
        slot, lo, hi = pieces[i]
        return pltpu.make_async_remote_copy(
            src_ref=own_x.at[lo:hi, :], dst_ref=halo.at[slot, lo:hi, :], send_sem=halo_send.at[i], recv_sem=halo_recv.at[i],
            device_id=(block + reach[i], part), device_id_type=MESH)

    def start_halo(i):
        target = block + reach[i]

        @pl.when((target >= 0) & (target < n_tm))
        def _():
            halo_copy(i).start()

    def sent_halo(i):
        target = block + reach[i]

        @pl.when((target >= 0) & (target < n_tm))
        def _():
            halo_copy(i).wait_send()

    def take_halo(slot):
        for i in range(len(pieces)):
            if pieces[i][0] == slot:
                origin = block - reach[i]

                @pl.when((origin >= 0) & (origin < n_tm))
                def _(i=i):
                    halo_copy(i).wait_recv()

    def place(upper, lower, at):
        xt[at:at + half, :] = jnp.concatenate([upper, lower], axis=0).T

    def base(step):
        return (STEPS - step) * rows

    def stats(step):
        lo = base(step)
        hi = lo + rows + (half if step == 0 else 0)
        span, level = 1, 0
        while span < half:
            last = min(hi, (STEPS + 2) * rows - half - 2 * span)
            last = lo + -(-(last - lo) // 8) * 8
            for at in range(lo, last, TILE):
                end = min(at + TILE, last)
                if span == 1:
                    here, later = xt[at:end, :], xt[at + span:end + span, :]
                else:
                    here, later = moments[level - 1, 0, at:end, :], moments[level - 1, 0, at + span:end + span, :]
                gap = later - here
                second = gap * gap * (0.5 / span)
                if span > 1:
                    second = second + (moments[level - 1, 1, at:end, :] + moments[level - 1, 1, at + span:end + span, :])
                moments[level, 0, at:end, :] = here + later
                moments[level, 1, at:end, :] = second
            span, level = 2 * span, level + 1
        for at in range(0, rows, TILE):
            here = moments[level - 1, 0, lo + at:lo + at + TILE, :]
            second = moments[level - 1, 1, lo + at:lo + at + TILE, :]
            later = pltpu.roll(here, depth, 1)
            gap = later - here
            second = second + pltpu.roll(second, depth, 1) + gap * gap * (0.5 / half)
            mu[step, at:at + TILE, :] = (here + later) * (1.0 / WIN)
            sc[step, at:at + TILE, :] = lax.rsqrt(second * (1.0 / WIN) + EPS)

    def build(step, g, target):
        for tile in range(0, rows, 16):
            m, s = mu[step, tile:tile + 16, :], sc[step, tile:tile + 16, :]
            for k in range(GROUP):
                z = (xt[pl.ds(base(step) + g * GROUP + (tile + k), 16), :] - m) * s
                target[k, tile:tile + 16, :] = z.astype(jnp.bfloat16)

    def product(weights, streamed):
        left = jnp.concatenate(
            [jnp.concatenate([z[k, 0:height, :] for z, height in streamed], axis=0) for k in range(GROUP)], axis=1)
        right = jnp.concatenate([weights[k] for k in range(GROUP)], axis=1)
        return lax.dot_general(left, right, (((1,), (1,)), ((), ())), preferred_element_type=jnp.float32)

    def send(step):
        own = heights[step] // n_chan
        copies = []
        for d in [*range(2, n_chan), 1]:
            at = pl.ds(pl.multiple_of(peer(d) * own, own), own)
            if d == 1:
                src, dst = acc.at[step, at, :], recv32.at[step, 0:own, :]
            else:
                send16[step, d - 2, 0:own, :] = acc[step, at, :].astype(jnp.bfloat16)
                src, dst = send16.at[step, d - 2, 0:own, :], recv16.at[step, d - 2, 0:own, :]
            copy = pltpu.make_async_remote_copy(
                src_ref=src, dst_ref=dst, send_sem=part_send.at[step, d - 1], recv_sem=part_recv.at[step, d - 1],
                device_id=(block, peer(d)), device_id_type=MESH)
            copy.start()
            copies.append(copy)
        return copies

    load.wait()
    start_halo(0)
    start_halo(1)
    place(own_x[:, :half], own_x[:, half:], base(0))
    pad = xt.shape[0] - ((STEPS + 2) * rows - half)
    xt[xt.shape[0] - pad:, :] = jnp.zeros((pad, lanes), jnp.float32)
    acc[...] = jnp.zeros_like(acc)
    sent_halo(0)
    start_halo(2)
    start_halo(3)
    take_halo(0)

    def arrive(step):
        if step == 0:
            early, late = own_x, jnp.where(block == n_tm - 1, 0.0, halo[0])
            place(late[:, :half], late[:, half:], base(0) + rows)
            place(early[:, half:], late[:, :half], base(0) + half)
        else:
            early, late = halo[step], own_x if step == 1 else halo[1]
            place(early[:, :half], early[:, half:], base(step))
            place(early[:, half:], late[:, :half], base(step) + half)

    sent = []
    pairs = chunks // 2
    low, mid = heights[0], heights[0] + heights[1]

    take = (low, heights[1], heights[2])

    def near(weights, mine, previous):
        return product(weights, [(mine, take[0]), (previous, take[1])])

    for step in range(2):
        if step == 1:
            take_halo(1)
        arrive(step)
        stats(step)
        build(step, 0, z0e.at[0] if step == 0 else z1e)
    take_halo(2)

    def add_near(first, second, fresh=False):
        for step, lo, hi in ((0, 0, low), (1, low, mid)):
            value = first[lo:hi] + second[lo:hi]
            acc[step, 0:hi - lo, :] = value if fresh else acc[step, 0:hi - lo, :] + value

    for h in range(EARLY):
        first = near(z0e.at[h], z0e.at[h], z1e)
        build(0, 2 * h + 1, z0o.at[h])
        build(1, 2 * h + 1, z1o)
        if h == 0:
            arrive(2)
        second = near(z0o.at[h], z0o.at[h], z1o)
        build(0, 2 * h + 2, z0e.at[h + 1])
        build(1, 2 * h + 2, z1e)
        if h == 0:
            stats(2)
        if h == EARLY - 1:
            build(2, 2 * h + 2, z2e)
        add_near(first, second, h == 0)

    def every(h, carry):
        first = product(z0e.at[h], [(z0e.at[h], take[0]), (z1e, take[1]), (z2e, take[2])])
        build(0, 2 * h + 1, z0o.at[h])
        build(1, 2 * h + 1, z1o)
        build(2, 2 * h + 1, z2o)
        second = product(z0o.at[h], [(z0o.at[h], take[0]), (z1o, take[1]), (z2o, take[2])])
        build(0, 2 * h + 2, z0e.at[h + 1])
        build(1, 2 * h + 2, z1e)
        build(2, lax.rem(2 * h + 2, chunks), z2e)
        add_near(first, second)
        acc[2] += first[mid:] + second[mid:]
        return carry

    lax.fori_loop(EARLY, pairs, every, 0)
    sent.append(send(0))
    sent.append(send(1))

    def far(h, carry):
        first = product(z0e.at[h], [(z2e, take[2])])
        build(2, 2 * h + 1, z2o)
        second = product(z0o.at[h], [(z2o, take[2])])
        build(2, 2 * h + 2, z2e)
        acc[2] += first + second
        return carry

    lax.fori_loop(0, EARLY, far, 0)
    sent.append(send(2))

    load_lengths.wait()

    def valid(which, local):
        seg_len = rows // 2
        limit = jnp.where(local < seg_len, lengths[which * 2], lengths[which * 2 + 1])
        offset = jnp.where(local < seg_len, local, local - seg_len)
        return (offset < limit) & (which * rows + local <= total - WIN)

    best = None
    for step in range(STEPS + 1):
        own = heights[step] // n_chan
        row_at = part * own + lax.broadcasted_iota(jnp.int32, (own, rows), 0)
        other = block - step
        safe = jnp.maximum(other, 0)
        col_at = lax.broadcasted_iota(jnp.int32, (own, rows), 1)
        keep = valid(block, col_at) & valid(safe, row_at) & (other >= 0) & (step * rows + col_at - row_at >= excl)
        for copy in sent[step]:
            copy.wait_recv()
        summed = acc[step, pl.ds(pl.multiple_of(part * own, own), own), :] + recv32[step, 0:own, :]
        for d in range(2, n_chan):
            summed = summed + recv16[step, d - 2, 0:own, :].astype(jnp.float32)
        top = jnp.max(jnp.where(keep, summed * (1.0 / WIN), MASKED), axis=0, keepdims=True)
        best = top if best is None else jnp.maximum(best, top)
    peaks[0] = best
    copies = []
    for d in range(1, n_chan):
        copy = pltpu.make_async_remote_copy(
            src_ref=peaks.at[0], dst_ref=peaks.at[d], send_sem=peak_send.at[d - 1], recv_sem=peak_recv.at[d - 1],
            device_id=(block, peer(d)), device_id_type=MESH)
        copy.start()
        copies.append(copy)
    for i in range(1, len(pieces)):
        sent_halo(i)
    for copy in [c for step in sent for c in step]:
        copy.wait_send()
    for copy in copies:
        copy.wait_recv()
    for d in range(1, n_chan):
        best = jnp.maximum(best, peaks[d])
    out[...] = jnp.where(best > 0.5 * MASKED, best, 0.0)

    for copy in copies:
        copy.wait_send()


def solution(mesh):
    n_tm, n_chan = mesh.shape["tm"], mesh.shape["chan"]

    def body(series, lengths):
        depth, rows = series.shape
        half = WIN // 2
        lanes = 2 * depth
        pairs = half // GROUP // 2
        high = (STEPS + 2) * rows - half + 16 + GROUP
        levels = half.bit_length() - 1
        own = rows // n_chan
        vmem = pl.BlockSpec(memory_space=pltpu.VMEM)
        peak = pl.pallas_call(
            functools.partial(kernel, n_tm, n_chan),
            out_shape=pltpu.VMEM((1, rows), jnp.float32),
            in_specs=[pl.BlockSpec(memory_space=pl.ANY), pl.BlockSpec(memory_space=pl.ANY)],
            out_specs=vmem,
            scratch_shapes=[
                pltpu.SMEM(lengths.shape, jnp.int32),
                pltpu.VMEM((depth, rows), jnp.float32),
                pltpu.VMEM((STEPS + 1, depth, rows), jnp.float32),
                pltpu.VMEM((high, lanes), jnp.float32),
                pltpu.VMEM((levels, 2, high, lanes), jnp.float32),
                pltpu.VMEM((STEPS + 1, rows, lanes), jnp.float32),
                pltpu.VMEM((STEPS + 1, rows, lanes), jnp.float32),
                pltpu.VMEM((pairs + 1, GROUP, rows, lanes), jnp.bfloat16),
                pltpu.VMEM((pairs, GROUP, rows, lanes), jnp.bfloat16),
                pltpu.VMEM((GROUP, rows, lanes), jnp.bfloat16),
                pltpu.VMEM((GROUP, rows, lanes), jnp.bfloat16),
                pltpu.VMEM((GROUP, rows, lanes), jnp.bfloat16),
                pltpu.VMEM((GROUP, rows, lanes), jnp.bfloat16),
                pltpu.VMEM((STEPS + 1, rows, rows), jnp.float32),
                pltpu.VMEM((STEPS + 1, n_chan - 2, own, rows), jnp.bfloat16),
                pltpu.VMEM((STEPS + 1, own, rows), jnp.float32),
                pltpu.VMEM((STEPS + 1, n_chan - 2, own, rows), jnp.bfloat16),
                pltpu.VMEM((n_chan, 1, rows), jnp.float32),
                pltpu.SemaphoreType.DMA,
                pltpu.SemaphoreType.DMA,
                pltpu.SemaphoreType.DMA((STEPS + 2,)),
                pltpu.SemaphoreType.DMA((STEPS + 2,)),
                pltpu.SemaphoreType.DMA((STEPS + 1, n_chan - 1)),
                pltpu.SemaphoreType.DMA((STEPS + 1, n_chan - 1)),
                pltpu.SemaphoreType.DMA((n_chan - 1,)),
                pltpu.SemaphoreType.DMA((n_chan - 1,)),
            ],
            compiler_params=pltpu.CompilerParams(collective_id=0, has_side_effects=True),
        )(lengths, series)
        return peak.reshape(rows)

    return jax.shard_map(
        body, mesh=mesh, in_specs=(P("chan", "tm"), P()), out_specs=P("tm"), check_vma=False)
```

```python
import functools

import jax
import jax.numpy as jnp
from jax import lax
from jax.experimental import pallas as pl
from jax.experimental.pallas import tpu as pltpu
from jax.sharding import PartitionSpec as P

WIN = 256
STEPS = 2
GROUP = 16
TILE = 32
EARLY = 2
EPS = 1e-05
MASKED = -1000000000.0
MESH = pl.DeviceIdType.MESH


def kernel(n_tm, n_chan, lengths_in, series, out, lengths, own_x, halo, xt, moments, mu, sc, z0e, z0o, z1e, z1o, z2e, z2o,
           acc, send16, recv32, recv16, peaks, load_sem, lengths_sem, halo_send, halo_recv, part_send, part_recv, peak_send, peak_recv):
    depth, rows = own_x.shape
    total = rows * n_tm
    excl = WIN // 4
    half = WIN // 2
    lanes = 2 * depth
    chunks = half // GROUP
    heights = [rows - excl] + [rows] * STEPS
    block = lax.axis_index("tm")
    part = lax.axis_index("chan")

    def peer(d):
        return jnp.bitwise_xor(part, d)

    load = pltpu.make_async_copy(series, own_x, load_sem)
    load.start()
    load_lengths = pltpu.make_async_copy(lengths_in, lengths, lengths_sem)
    load_lengths.start()

    barrier = pltpu.get_barrier_semaphore()
    for distance in (1, -1, -2):
        target = block + distance

        @pl.when((target >= 0) & (target < n_tm))
        def _(target=target):
            pl.semaphore_signal(barrier, inc=1, device_id=(target, part), device_id_type=MESH)

    for d in range(1, n_chan):
        pl.semaphore_signal(barrier, inc=1, device_id=(block, peer(d)), device_id_type=MESH)
    greeted = n_chan - 1
    for distance in (-1, 1, 2):
        target = block + distance
        greeted = greeted + jnp.where((target >= 0) & (target < n_tm), 1, 0)
    pl.semaphore_wait(barrier, greeted)

    reach = (-1, -1, 1, 2)
    pieces = ((0, 0, depth // 4), (0, depth // 4, depth), (1, 0, depth), (2, 0, depth))

    def halo_copy(i):
        slot, lo, hi = pieces[i]
        return pltpu.make_async_remote_copy(
            src_ref=own_x.at[lo:hi, :], dst_ref=halo.at[slot, lo:hi, :], send_sem=halo_send.at[i], recv_sem=halo_recv.at[i],
            device_id=(block + reach[i], part), device_id_type=MESH)

    def start_halo(i):
        target = block + reach[i]

        @pl.when((target >= 0) & (target < n_tm))
        def _():
            halo_copy(i).start()

    def sent_halo(i):
        target = block + reach[i]

        @pl.when((target >= 0) & (target < n_tm))
        def _():
            halo_copy(i).wait_send()

    def take_halo(slot):
        for i in range(len(pieces)):
            if pieces[i][0] == slot:
                origin = block - reach[i]

                @pl.when((origin >= 0) & (origin < n_tm))
                def _(i=i):
                    halo_copy(i).wait_recv()

    def place(upper, lower, at):
        xt[at:at + half, :] = jnp.concatenate([upper, lower], axis=0).T

    def base(step):
        return (STEPS - step) * rows

    def stats(step):
        lo = base(step)
        hi = lo + rows + (half if step == 0 else 0)
        span, level = 1, 0
        while span < half:
            last = min(hi, (STEPS + 2) * rows - half - 2 * span)
            last = lo + -(-(last - lo) // 8) * 8
            for at in range(lo, last, TILE):
                end = min(at + TILE, last)
                if span == 1:
                    here, later = xt[at:end, :], xt[at + span:end + span, :]
                else:
                    here, later = moments[level - 1, 0, at:end, :], moments[level - 1, 0, at + span:end + span, :]
                gap = later - here
                second = gap * gap * (0.5 / span)
                if span > 1:
                    second = second + (moments[level - 1, 1, at:end, :] + moments[level - 1, 1, at + span:end + span, :])
                moments[level, 0, at:end, :] = here + later
                moments[level, 1, at:end, :] = second
            span, level = 2 * span, level + 1
        for at in range(0, rows, TILE):
            here = moments[level - 1, 0, lo + at:lo + at + TILE, :]
            second = moments[level - 1, 1, lo + at:lo + at + TILE, :]
            later = pltpu.roll(here, depth, 1)
            gap = later - here
            second = second + pltpu.roll(second, depth, 1) + gap * gap * (0.5 / half)
            mu[step, at:at + TILE, :] = (here + later) * (1.0 / WIN)
            sc[step, at:at + TILE, :] = lax.rsqrt(second * (1.0 / WIN) + EPS)

    def build(step, g, target):
        for tile in range(0, rows, 16):
            m, s = mu[step, tile:tile + 16, :], sc[step, tile:tile + 16, :]
            for k in range(GROUP):
                z = (xt[pl.ds(base(step) + g * GROUP + (tile + k), 16), :] - m) * s
                target[k, tile:tile + 16, :] = z.astype(jnp.bfloat16)

    def product(weights, streamed):
        left = jnp.concatenate(
            [jnp.concatenate([z[k, 0:height, :] for z, height in streamed], axis=0) for k in range(GROUP)], axis=1)
        right = jnp.concatenate([weights[k] for k in range(GROUP)], axis=1)
        return lax.dot_general(left, right, (((1,), (1,)), ((), ())), preferred_element_type=jnp.float32)

    def send(step):
        own = heights[step] // n_chan
        copies = []
        for d in [*range(2, n_chan), 1]:
            at = pl.ds(pl.multiple_of(peer(d) * own, own), own)
            if d == 1:
                src, dst = acc.at[step, at, :], recv32.at[step, 0:own, :]
            else:
                send16[step, d - 2, 0:own, :] = acc[step, at, :].astype(jnp.bfloat16)
                src, dst = send16.at[step, d - 2, 0:own, :], recv16.at[step, d - 2, 0:own, :]
            copy = pltpu.make_async_remote_copy(
                src_ref=src, dst_ref=dst, send_sem=part_send.at[step, d - 1], recv_sem=part_recv.at[step, d - 1],
                device_id=(block, peer(d)), device_id_type=MESH)
            copy.start()
            copies.append(copy)
        return copies

    load.wait()
    start_halo(0)
    start_halo(1)
    place(own_x[:, :half], own_x[:, half:], base(0))
    pad = xt.shape[0] - ((STEPS + 2) * rows - half)
    xt[xt.shape[0] - pad:, :] = jnp.zeros((pad, lanes), jnp.float32)
    acc[...] = jnp.zeros_like(acc)
    sent_halo(0)
    start_halo(2)
    start_halo(3)
    take_halo(0)

    def arrive(step):
        if step == 0:
            early, late = own_x, jnp.where(block == n_tm - 1, 0.0, halo[0])
            place(late[:, :half], late[:, half:], base(0) + rows)
            place(early[:, half:], late[:, :half], base(0) + half)
        else:
            early, late = halo[step], own_x if step == 1 else halo[1]
            place(early[:, :half], early[:, half:], base(step))
            place(early[:, half:], late[:, :half], base(step) + half)

    sent = []
    pairs = chunks // 2
    low, mid = heights[0], heights[0] + heights[1]

    take = (low, heights[1], heights[2])

    def near(weights, mine, previous):
        return product(weights, [(mine, take[0]), (previous, take[1])])

    for step in range(2):
        if step == 1:
            take_halo(1)
        arrive(step)
        stats(step)
        build(step, 0, z0e.at[0] if step == 0 else z1e)
    take_halo(2)

    def add_near(first, second, fresh=False):
        for step, lo, hi in ((0, 0, low), (1, low, mid)):
            value = first[lo:hi] + second[lo:hi]
            acc[step, 0:hi - lo, :] = value if fresh else acc[step, 0:hi - lo, :] + value

    for h in range(EARLY):
        first = near(z0e.at[h], z0e.at[h], z1e)
        build(0, 2 * h + 1, z0o.at[h])
        build(1, 2 * h + 1, z1o)
        if h == 0:
            arrive(2)
        second = near(z0o.at[h], z0o.at[h], z1o)
        build(0, 2 * h + 2, z0e.at[h + 1])
        build(1, 2 * h + 2, z1e)
        if h == 0:
            stats(2)
        if h == EARLY - 1:
            build(2, 2 * h + 2, z2e)
        add_near(first, second, h == 0)

    def every(h, carry):
        first = product(z0e.at[h], [(z0e.at[h], take[0]), (z1e, take[1]), (z2e, take[2])])
        build(0, 2 * h + 1, z0o.at[h])
        build(1, 2 * h + 1, z1o)
        build(2, 2 * h + 1, z2o)
        second = product(z0o.at[h], [(z0o.at[h], take[0]), (z1o, take[1]), (z2o, take[2])])
        build(0, 2 * h + 2, z0e.at[h + 1])
        build(1, 2 * h + 2, z1e)
        build(2, lax.rem(2 * h + 2, chunks), z2e)
        add_near(first, second)
        acc[2] += first[mid:] + second[mid:]
        return carry

    lax.fori_loop(EARLY, pairs, every, 0)
    sent.append(send(0))
    sent.append(send(1))

    def far(h, carry):
        first = product(z0e.at[h], [(z2e, take[2])])
        build(2, 2 * h + 1, z2o)
        second = product(z0o.at[h], [(z2o, take[2])])
        build(2, 2 * h + 2, z2e)
        acc[2] += first + second
        return carry

    lax.fori_loop(0, EARLY, far, 0)
    sent.append(send(2))

    load_lengths.wait()

    def valid(which, local):
        seg_len = rows // 2
        limit = jnp.where(local < seg_len, lengths[which * 2], lengths[which * 2 + 1])
        offset = jnp.where(local < seg_len, local, local - seg_len)
        return (offset < limit) & (which * rows + local <= total - WIN)

    best = None
    for step in range(STEPS + 1):
        own = heights[step] // n_chan
        row_at = part * own + lax.broadcasted_iota(jnp.int32, (own, rows), 0)
        other = block - step
        safe = jnp.maximum(other, 0)
        col_at = lax.broadcasted_iota(jnp.int32, (own, rows), 1)
        keep = valid(block, col_at) & valid(safe, row_at) & (other >= 0) & (step * rows + col_at - row_at >= excl)
        for copy in sent[step]:
            copy.wait_recv()
        summed = acc[step, pl.ds(pl.multiple_of(part * own, own), own), :] + recv32[step, 0:own, :]
        for d in range(2, n_chan):
            summed = summed + recv16[step, d - 2, 0:own, :].astype(jnp.float32)
        top = jnp.max(jnp.where(keep, summed * (1.0 / WIN), MASKED), axis=0, keepdims=True)
        best = top if best is None else jnp.maximum(best, top)
    peaks[0] = best
    copies = []
    for d in range(1, n_chan):
        copy = pltpu.make_async_remote_copy(
            src_ref=peaks.at[0], dst_ref=peaks.at[d], send_sem=peak_send.at[d - 1], recv_sem=peak_recv.at[d - 1],
            device_id=(block, peer(d)), device_id_type=MESH)
        copy.start()
        copies.append(copy)
    for i in range(1, len(pieces)):
        sent_halo(i)
    for copy in [c for step in sent for c in step] + copies:
        copy.wait_send()
    for copy in copies:
        copy.wait_recv()
    for d in range(1, n_chan):
        best = jnp.maximum(best, peaks[d])
    out[...] = jnp.where(best > 0.5 * MASKED, best, 0.0)


def solution(mesh):
    n_tm, n_chan = mesh.shape["tm"], mesh.shape["chan"]

    def body(series, lengths):
        depth, rows = series.shape
        half = WIN // 2
        lanes = 2 * depth
        pairs = half // GROUP // 2
        high = (STEPS + 2) * rows - half + 16 + GROUP
        levels = half.bit_length() - 1
        own = rows // n_chan
        vmem = pl.BlockSpec(memory_space=pltpu.VMEM)
        peak = pl.pallas_call(
            functools.partial(kernel, n_tm, n_chan),
            out_shape=pltpu.VMEM((1, rows), jnp.float32),
            in_specs=[pl.BlockSpec(memory_space=pl.ANY), pl.BlockSpec(memory_space=pl.ANY)],
            out_specs=vmem,
            scratch_shapes=[
                pltpu.SMEM(lengths.shape, jnp.int32),
                pltpu.VMEM((depth, rows), jnp.float32),
                pltpu.VMEM((STEPS + 1, depth, rows), jnp.float32),
                pltpu.VMEM((high, lanes), jnp.float32),
                pltpu.VMEM((levels, 2, high, lanes), jnp.float32),
                pltpu.VMEM((STEPS + 1, rows, lanes), jnp.float32),
                pltpu.VMEM((STEPS + 1, rows, lanes), jnp.float32),
                pltpu.VMEM((pairs + 1, GROUP, rows, lanes), jnp.bfloat16),
                pltpu.VMEM((pairs, GROUP, rows, lanes), jnp.bfloat16),
                pltpu.VMEM((GROUP, rows, lanes), jnp.bfloat16),
                pltpu.VMEM((GROUP, rows, lanes), jnp.bfloat16),
                pltpu.VMEM((GROUP, rows, lanes), jnp.bfloat16),
                pltpu.VMEM((GROUP, rows, lanes), jnp.bfloat16),
                pltpu.VMEM((STEPS + 1, rows, rows), jnp.float32),
                pltpu.VMEM((STEPS + 1, n_chan - 2, own, rows), jnp.bfloat16),
                pltpu.VMEM((STEPS + 1, own, rows), jnp.float32),
                pltpu.VMEM((STEPS + 1, n_chan - 2, own, rows), jnp.bfloat16),
                pltpu.VMEM((n_chan, 1, rows), jnp.float32),
                pltpu.SemaphoreType.DMA,
                pltpu.SemaphoreType.DMA,
                pltpu.SemaphoreType.DMA((STEPS + 2,)),
                pltpu.SemaphoreType.DMA((STEPS + 2,)),
                pltpu.SemaphoreType.DMA((STEPS + 1, n_chan - 1)),
                pltpu.SemaphoreType.DMA((STEPS + 1, n_chan - 1)),
                pltpu.SemaphoreType.DMA((n_chan - 1,)),
                pltpu.SemaphoreType.DMA((n_chan - 1,)),
            ],
            compiler_params=pltpu.CompilerParams(collective_id=0, has_side_effects=True),
        )(lengths, series)
        return peak.reshape(rows)

    return jax.shard_map(
        body, mesh=mesh, in_specs=(P("chan", "tm"), P()), out_specs=P("tm"), check_vma=False)
```
